256 devices in a mesh: blk: 16 (over x_lo, z), dp: 16 (over x_hi, y, core).
Axes of the slice: x: 4 (x_hi: 2, x_lo: 2; x = x_hi * 2 + x_lo), y: 4, z: 8, core: 2. Of those that a mesh axis runs over, the one named last changes fastest.
Arguments:
- tokens: bfloat16 [32768, 3072], P(('blk', 'dp')), may hold values from -6 to 6
- expert_ids: int32 [32768, 2], P(('blk', 'dp')), may hold values from 0 to 7, as said below
- gate_num: int32 [32768], P(('blk', 'dp')), may hold values from 1 to 255
- gate_weight: bfloat16 [3072, 8192], P('dp', 'blk'), may hold values from -0.109375 to 0.109375
- up_weight: bfloat16 [3072, 8192], P('dp', 'blk'), may hold values from -0.109375 to 0.109375
- down_weight: bfloat16 [8192, 3072], P(('blk', 'dp')), may hold values from -0.0625 to 0.0625
Outputs:
- moe_out: bfloat16 [32768, 3072], P(('blk', 'dp'))
The draws below stay inside these ranges and needn't reach their ends.
Inputs may be any that keep to these rules, and one draw needn't show every extreme that they name: `expert_ids`: each row names two different experts. Among the 128 rows of one device (aligned blocks), between 1 and 64 name expert 0, and in every draw the rows of some device include exactly 64 such rows.
All inputs are finite; a program needn't handle non-finite values.
Results may differ from the reference program's by a relative error of at most 0.018.
Values may be sent and summed in bfloat16 or wider, within the bound.
No kernel may reach another device: no remote copies, remote signals or barrier semaphores. Data moves between devices by JAX's collectives and lax.ppermute only.
A program may use at most 192 MiB of HBM per device.

```python
import jax
import jax.numpy as jnp
from jax import lax

D = 3072
FF = 8192
EXPERTS = 8
T_DEV = 128
CAP = 64
TOKENS = 32768
N_BLK = 16
N_DP = 16


def draw_expert_ids(key, part):
    blocks = TOKENS // T_DEV
    keys = jax.random.split(jax.random.fold_in(key, 11), 6)
    loads = jax.random.randint(keys[0], (blocks,), 1, CAP + 1)
    fullest = jax.random.randint(keys[1], (), 0, blocks)
    loads = jnp.where(jnp.arange(blocks) == fullest, CAP, loads)
    scores = jax.random.randint(keys[2], (blocks, T_DEV), 0, 1 << 20) * T_DEV + jnp.arange(T_DEV)[None, :]
    ranks = jnp.argsort(jnp.argsort(scores, axis=1), axis=1)
    chosen = ranks < loads[:, None]
    other_first = jax.random.randint(keys[3], (blocks, T_DEV), 1, EXPERTS)
    offset = jax.random.randint(keys[4], (blocks, T_DEV), 1, EXPERTS - 1)
    other_second = (other_first - 1 + offset) % (EXPERTS - 1) + 1
    first = jnp.where(chosen, 0, other_first)
    second = jnp.where(chosen, other_first, other_second)
    flipped = jax.random.randint(keys[5], (blocks, T_DEV), 0, 2) == 1
    left = jnp.where(flipped, second, first)
    right = jnp.where(flipped, first, second)
    return jnp.stack([left, right], axis=-1).reshape(TOKENS, 2).astype(jnp.int32)


def touch_ends(values, rng, smallest, top_value):
    spot = [jax.random.randint(jax.random.fold_in(rng, axis), (), 0, length) for axis, length in enumerate(values.shape)]
    main_axis = values.shape.index(max(values.shape))
    next_to = spot[:main_axis] + [(spot[main_axis] + 1) % values.shape[main_axis]] + spot[main_axis + 1:]
    return values.at[tuple(spot)].set(smallest).at[tuple(next_to)].set(top_value)


def steps_of(stream_key, dims, cuts, least, high):
    def one(dim, blocks):
        steps = jax.random.uniform(jax.random.fold_in(jax.random.fold_in(stream_key, 6), dim), (blocks,), jnp.float32, least / len(cuts), high / len(cuts))
        return jnp.repeat(jnp.exp(steps), dims[dim] // blocks).reshape((-1,) + (1,) * (len(dims) - dim - 1))

    gain = one(*cuts[0])
    for cut in cuts[1:]:
        gain = gain * one(*cut)
    return gain


def normal_values(own_key, shape, spread, most, cuts=(), held_as=jnp.bfloat16):
    drawn = spread * jax.random.normal(own_key, shape, jnp.float32)
    if cuts:
        drawn = drawn * steps_of(own_key, shape, cuts, -0.22, 0.18)
    return jnp.clip(drawn, -most, most).astype(held_as)


def setup_inputs(seed: int = 0) -> dict:
    streams_of = jax.random.split(jax.random.key(seed), 7)
    return {
        "tokens": normal_values(streams_of[0], (TOKENS, D), 1.0, 6.0, ((0, 256),)),
        "expert_ids": draw_expert_ids(jax.random.fold_in(streams_of[6], 71), 0),
        "gate_num": touch_ends(jax.random.randint(streams_of[2], (TOKENS,), 1, 256), jax.random.fold_in(streams_of[2], 1), 1, 255).astype(jnp.int32),
        "gate_weight": normal_values(streams_of[3], (D, FF), D ** -0.5, 0.109375, ((0, 16), (1, 16))),
        "up_weight": normal_values(streams_of[4], (D, FF), D ** -0.5, 0.109375, ((0, 16), (1, 16))),
        "down_weight": normal_values(streams_of[5], (FF, D), FF ** -0.5, 0.0625, ((0, 256),)),
    }


GATE_SCALE = 256.0


def route_table(expert_ids, slot_count):
    hits = jnp.sum((expert_ids == 0).astype(jnp.int32), axis=1)
    position = jnp.cumsum(hits) - 1
    marks = (hits[:, None] > 0) & (position[:, None] == jnp.arange(slot_count, dtype=jnp.int32)[None, :])
    return marks.astype(jnp.float32)


def gate_values(expert_ids, gate_num):
    first = gate_num.astype(jnp.float32) / GATE_SCALE
    return jnp.where(expert_ids[:, 0] == 0, first, 0.0) + jnp.where(expert_ids[:, 1] == 0, 1.0 - first, 0.0)


def reference(tokens, expert_ids, gate_num, gate_weight, up_weight, down_weight):
    slot_count = T_DEV // 2
    block_len = FF // N_BLK
    grouped_x = tokens.reshape(N_BLK, N_DP, T_DEV, D)
    grouped_ids = expert_ids.reshape(N_BLK, N_DP, T_DEV, 2)
    grouped_num = gate_num.reshape(N_BLK, N_DP, T_DEV)

    def one_group(inputs):
        block_x, block_ids, block_num = inputs
        marks = jax.vmap(lambda ids: route_table(ids, slot_count))(block_ids)
        packed = jnp.einsum("btc,btd->bcd", marks, block_x.astype(jnp.float32)).astype(jnp.bfloat16)
        packed = packed.reshape(N_DP * slot_count, D)
        gate = jnp.dot(packed, gate_weight, preferred_element_type=jnp.float32)
        up = jnp.dot(packed, up_weight, preferred_element_type=jnp.float32)
        hidden = (jax.nn.silu(gate) * up).astype(jnp.bfloat16)

        def add_block(running, index):
            start = (index * block_len).astype(jnp.int32)
            columns = lax.dynamic_slice_in_dim(hidden, start, block_len, 1)
            rows = lax.dynamic_slice_in_dim(down_weight, start, block_len, 0)
            term = jnp.dot(columns, rows, preferred_element_type=jnp.float32).astype(jnp.bfloat16)
            term = lax.optimization_barrier(term)
            return running + term.astype(jnp.float32), None

        rows_out, _ = lax.scan(add_block, jnp.zeros((N_DP * slot_count, D), jnp.float32), jnp.arange(N_BLK, dtype=jnp.int32))
        rows_out = rows_out.reshape(N_DP, slot_count, D)
        expanded = jnp.einsum("btc,bcd->btd", marks, rows_out, precision=lax.Precision.HIGHEST)
        weights = jax.vmap(gate_values)(block_ids, block_num)
        return (weights[:, :, None] * expanded).astype(jnp.bfloat16)

    result = lax.map(one_group, (grouped_x, grouped_ids, grouped_num))
    return result.reshape(TOKENS, D)
```

```python
import jax
import jax.numpy as jnp
from jax import lax
from jax.experimental import pallas as pl
from jax.experimental.pallas import tpu as pltpu
from jax.sharding import PartitionSpec as P

GATE_SCALE = 256.0
AXES = ("blk", "dp")
BF = jnp.bfloat16
F32 = jnp.float32

NX, NY, NZ = 4, 4, 8


def shift(a, dx=0, dy=0, dz=0, other_core=False):
    pairs = []
    for i in range(256):
        xl, z, xh, y, c = i // 128, i // 16 % 8, i // 8 % 2, i // 2 % 4, i % 2
        x = (2 * xh + xl + dx) % NX
        y = (y + dy) % NY
        z = (z + dz) % NZ
        c = 1 - c if other_core else c
        pairs.append((i, (x % 2) * 128 + z * 16 + (x // 2) * 8 + y * 2 + c))
    return lax.ppermute(a, AXES, pairs)


def route_table(expert_ids, slot_count):
    hits = jnp.sum((expert_ids == 0).astype(jnp.int32), axis=1)
    position = jnp.cumsum(hits) - 1
    marks = (hits[:, None] > 0) & (
        position[:, None] == jnp.arange(slot_count, dtype=jnp.int32)[None, :]
    )
    return marks.astype(BF)


def gate_values(expert_ids, gate_num):
    first = gate_num.astype(F32) / GATE_SCALE
    return jnp.where(expert_ids[:, 0] == 0, first, 0.0) + jnp.where(
        expert_ids[:, 1] == 0, 1.0 - first, 0.0
    )


def ring4(a, axis, cut):
    low = shift(a, **{axis: 1})
    high = shift(a, **{axis: -1})
    far_a = shift(low[:cut], **{axis: 1})
    far_b = shift(high[cut:], **{axis: -1})
    return a, low, far_a, far_b, high


RING_PARTS = ((0, 0, (0, 1, 2, 3)), (1, 1, (0, 1, 2, 3)), (2, 2, (0, 1)), (3, 2, (2, 3)), (4, 3, (0, 1, 2, 3)))
STEPS = (0, -1, 2, 1)


def places(x, y):
    return [[((STEPS[i] % 2), (x + STEPS[i]) % NX // 2, (y + STEPS[j]) % NY) for j in range(4)] for i in range(4)]


def hidden_kernel(pos, tok, *refs):
    gates, ups = refs[:5], refs[5:10]
    out, wg, wu, sems = refs[10:]
    x, y = pos[0], pos[1]
    where = places(x, y)
    copies = []
    for which, (arrays, dst) in enumerate(((gates, wg), (ups, wu))):
        for n, outer, inner in RING_PARTS:
            for at, q in enumerate(inner):
                i, j = (q, outer) if which == 0 else (outer, q)
                parity, xh, yy = where[i][j]
                row = pl.multiple_of((xh * NY + yy) * 384, 384)
                copies.append(pltpu.make_async_copy(
                    arrays[n].at[pl.ds(at * 384, 384)], dst.at[parity, pl.ds(row, 384)], sems.at[len(copies)]))
    for cp in copies:
        cp.start()
    for cp in copies:
        cp.wait()

    def rows(m, _):
        r = pl.ds(pl.multiple_of(m * 256, 256), 256)
        t = tok[r, :]
        for p in range(2):
            g = jnp.dot(t, wg[p], preferred_element_type=F32)
            u = jnp.dot(t, wu[p], preferred_element_type=F32)
            out[r, pl.ds(p * 256, 256)] = (g / (1.0 + jnp.exp(-g)) * u).astype(BF)
        return _

    lax.fori_loop(0, 4, rows, 0)


def down_kernel(pos, own, other, *refs):
    first, second = refs[:5], refs[5:10]
    out, wd, sems = refs[10:]
    x, y, c = pos[0], pos[1], pos[2]
    where = places(x, y)
    copies = []
    for which, arrays in enumerate((first, second)):
        for n, outer, inner in RING_PARTS:
            for at, q in enumerate(inner):
                i, j = (q, outer) if which == 0 else (outer, q)
                parity, xh, yy = where[i][j]
                row = pl.multiple_of(jnp.where(xh == c, 0, 256) + yy * 64, 64)
                copies.append(pltpu.make_async_copy(
                    arrays[n].at[pl.ds(at * 3, 3)],
                    wd.at[parity, pl.ds(which * 3, 3), pl.ds(row, 64)], sems.at[len(copies)]))
    for cp in copies:
        cp.start()
    for cp in copies:
        cp.wait()

    def rows(m, _):
        r = pl.ds(pl.multiple_of(m * 256, 256), 256)
        swapped = jnp.concatenate(
            [other[pl.ds(pl.multiple_of(m * 256 + at, 64), 64), :] for at in (64, 0, 192, 128)], axis=0)
        h = [jnp.concatenate([own[r, pl.ds(p * 256, 256)], swapped[:, p * 256:p * 256 + 256]], axis=1) for p in range(2)]
        for n in range(6):
            s = jnp.dot(h[0], wd[0, n], preferred_element_type=F32) + jnp.dot(h[1], wd[1, n], preferred_element_type=F32)
            out[r, pl.ds(n * 256, 256)] = s.astype(BF)
        return _

    lax.fori_loop(0, 4, rows, 0)


def call(kernel, pos, vmem, hbm, out_shape, scratch, flops, name):
    return pl.pallas_call(
        kernel,
        out_shape=jax.ShapeDtypeStruct(out_shape, BF),
        in_specs=[pl.BlockSpec(memory_space=pltpu.SMEM)]
        + [pl.BlockSpec(memory_space=pltpu.VMEM)] * len(vmem)
        + [pl.BlockSpec(memory_space=pl.ANY)] * len(hbm),
        out_specs=pl.BlockSpec(memory_space=pltpu.VMEM),
        scratch_shapes=[pltpu.VMEM(s, BF) for s in scratch] + [pltpu.SemaphoreType.DMA((32,))],
        compiler_params=pltpu.CompilerParams(vmem_limit_bytes=48 * 1024 * 1024),
        cost_estimate=pl.CostEstimate(flops=flops, bytes_accessed=12 << 20, transcendentals=0),
        name=name,
    )(pos, *vmem, *hbm)


def on_device(tokens, expert_ids, gate_num, gate_weight, up_weight, down_weight):
    blk, dp = lax.axis_index("blk"), lax.axis_index("dp")
    core = dp % 2
    x = dp // 8 * 2 + blk // 8
    y = dp // 2 % 4
    pos = jnp.stack([x, y, core]).astype(jnp.int32)
    even = core == 0

    def halves(h):
        g = lax.dynamic_slice_in_dim(gate_weight, h * 256, 256, 1).reshape(6, 32, 256)
        u = lax.dynamic_slice_in_dim(up_weight, h * 256, 256, 1).reshape(6, 32, 256)
        d = lax.dynamic_slice_in_dim(down_weight, h * 1536, 1536, 1).reshape(32, 6, 256).transpose(1, 0, 2)
        return jnp.concatenate([g, u, d], axis=0)

    keep = halves(core)
    got = shift(halves(1 - core), other_core=True)
    lo = jnp.where(even, keep, got)
    hi = jnp.where(even, got, keep)

    def stacked(k):
        return jnp.concatenate([lo[k:k + 6].reshape(192, 256), hi[k:k + 6].reshape(192, 256)], axis=0).reshape(6, 64, 256)

    down = jnp.concatenate([lo[12:], hi[12:]], axis=1)
    by_x = ring4(jnp.concatenate([stacked(0), down[:3]], axis=0), "dx", 5)
    by_y = ring4(jnp.concatenate([stacked(6), down[3:]], axis=0), "dy", 5)

    def bundles(r):
        far = jnp.concatenate([r[2], r[3]], axis=0)
        four = (r[0], r[1], far, r[4])
        return jnp.concatenate([a[:6] for a in four], axis=0), jnp.concatenate([a[6:] for a in four], axis=0)

    gate_b, down_a = bundles(by_x)
    up_b, down_b = bundles(by_y)
    gates = ring4(gate_b, "dy", 12)
    ups = ring4(up_b, "dx", 12)
    downs_a = ring4(down_a, "dy", 6)
    downs_b = ring4(down_b, "dx", 6)

    marks = route_table(expert_ids, 64)
    packed = lax.dot_general(
        marks, tokens, (((0,), (0,)), ((), ())), preferred_element_type=F32
    ).astype(BF)
    below, above = [packed], [packed]
    for s in range(3):
        below.append(shift(below[-1], dz=1))
        above.append(shift(above[-1], dz=-1))
    far_a = shift(below[3][:32], dz=1)
    far_b = shift(above[3][32:], dz=-1)
    chunks = [[far_a, far_b], [above[3]], [below[3]], [above[2]], [below[2]], [above[1]], [below[1]], [packed]]
    rows = []
    for chunk in chunks:
        rows += chunk + [shift(a, other_core=True) for a in chunk]
    together = jnp.concatenate(rows, axis=0)

    flat = [a.reshape(-1, 256) for a in gates + ups]
    hidden = call(hidden_kernel, pos, [together], flat, (1024, 512), [(2, 3072, 256), (2, 3072, 256)],
                  2 * 1024 * 3072 * 1024, "hidden")
    other = shift(hidden, other_core=True)
    term = call(down_kernel, pos, [hidden, other], list(downs_a + downs_b), (1024, 1536), [(2, 6, 512, 256)],
                2 * 1024 * 1024 * 1536, "down")

    def part(i):
        return term[128 * i:128 * i + 128].astype(F32)

    up_sum = shift(term[:64], dz=1)
    down_sum = shift(term[64:128], dz=-1)
    pad = jnp.zeros((64, 1536), BF)
    up_sum = jnp.concatenate([up_sum, pad], axis=0)
    down_sum = jnp.concatenate([pad, down_sum], axis=0)
    for s in range(3):
        up_sum = shift((part(1 + 2 * s) + up_sum.astype(F32)).astype(BF), dz=1)
        down_sum = shift((part(2 + 2 * s) + down_sum.astype(F32)).astype(BF), dz=-1)
    total = (part(7) + up_sum.astype(F32) + down_sum.astype(F32)).astype(BF)
    mine = total[:64]
    theirs = shift(total[64:], other_core=True)
    own_rows = jnp.concatenate([jnp.where(even, mine, theirs), jnp.where(even, theirs, mine)], axis=1)
    expanded = jnp.dot(marks, own_rows, preferred_element_type=F32)
    weights = gate_values(expert_ids, gate_num)
    return (weights[:, None] * expanded).astype(BF)


def solution(mesh):
    return jax.shard_map(
        on_device,
        mesh=mesh,
        in_specs=(
            P(("blk", "dp"), None),
            P(("blk", "dp"), None),
            P(("blk", "dp")),
            P("dp", "blk"),
            P("dp", "blk"),
            P(("blk", "dp"), None),
        ),
        out_specs=P(("blk", "dp"), None),
        check_vma=False,
    )
```

```python
import jax
import jax.numpy as jnp
from jax import lax
from jax.experimental import pallas as pl
from jax.experimental.pallas import tpu as pltpu
from jax.sharding import PartitionSpec as P

GATE_SCALE = 256.0
AXES = ("blk", "dp")
BF = jnp.bfloat16
F32 = jnp.float32

NX, NY, NZ = 4, 4, 8


def shift(a, dx=0, dy=0, dz=0, other_core=False):
    pairs = []
    for i in range(256):
        xl, z, xh, y, c = i // 128, i // 16 % 8, i // 8 % 2, i // 2 % 4, i % 2
        x = (2 * xh + xl + dx) % NX
        y = (y + dy) % NY
        z = (z + dz) % NZ
        c = 1 - c if other_core else c
        pairs.append((i, (x % 2) * 128 + z * 16 + (x // 2) * 8 + y * 2 + c))
    return lax.ppermute(a, AXES, pairs)


def device(xl, z, xh, y, c):
    return xl * 128 + z * 16 + xh * 8 + y * 2 + c


PLANES = [
    [device(x % 2, z, x // 2, y, c) for x in range(4) for y in range(4) for c in range(2)] for z in range(8)
]


def route_table(expert_ids, slot_count):
    hits = jnp.sum((expert_ids == 0).astype(jnp.int32), axis=1)
    position = jnp.cumsum(hits) - 1
    marks = (hits[:, None] > 0) & (
        position[:, None] == jnp.arange(slot_count, dtype=jnp.int32)[None, :]
    )
    return marks.astype(BF)


def gate_values(expert_ids, gate_num):
    first = gate_num.astype(F32) / GATE_SCALE
    return jnp.where(expert_ids[:, 0] == 0, first, 0.0) + jnp.where(
        expert_ids[:, 1] == 0, 1.0 - first, 0.0
    )


def ring4(a, axis, cut):
    low = shift(a, **{axis: 1})
    high = shift(a, **{axis: -1})
    far_a = shift(low[:cut], **{axis: 1})
    far_b = shift(high[cut:], **{axis: -1})
    return a, low, far_a, far_b, high


RING_PARTS = ((0, 0, (0, 1, 2, 3)), (1, 1, (0, 1, 2, 3)), (2, 2, (0, 1)), (3, 2, (2, 3)), (4, 3, (0, 1, 2, 3)))
STEPS = (0, -1, 2, 1)


def hidden_kernel(pos, tok, weights, out, w, sems):
    c = pos[2]
    copies = []
    for xl in range(2):
        for which in range(2):
            col = pl.multiple_of(which * 512 + c * 256, 256)
            for xh in range(2):
                copies.append(pltpu.make_async_copy(
                    weights.at[pl.ds((xh * 2 + xl) * 1536, 1536), pl.ds(col, 256)],
                    w.at[xl, pl.ds(xh * 1536, 1536), pl.ds(which * 256, 256)], sems.at[len(copies)]))
    for cp in copies:
        cp.start()
    for xl in range(2):
        for cp in copies[4 * xl:4 * xl + 4]:
            cp.wait()

        def rows(m, _):
            r = pl.ds(pl.multiple_of(m * 256, 256), 256)
            s = jnp.dot(tok[r, :], w[xl], preferred_element_type=F32)
            g, u = s[:, :256], s[:, 256:]
            out[r, pl.ds(xl * 256, 256)] = (g / (1.0 + jnp.exp(-g)) * u).astype(BF)
            return _

        lax.fori_loop(0, 4, rows, 0)


def down_kernel(pos, own, other, *refs):
    first, second = refs[:5], refs[5:10]
    out, wd, sems = refs[10:]
    x, y, c = pos[0], pos[1], pos[2]
    copies = []
    for which, arrays in enumerate((first, second)):
        for n, outer, inner in RING_PARTS:
            for at, q in enumerate(inner):
                i, j = (q, outer) if which == 0 else (outer, q)
                xs, ys = (x + STEPS[i]) % NX, (y + STEPS[j]) % NY
                row = pl.multiple_of(jnp.where(xs // 2 == c, 0, 256) + ys * 64, 64)
                copies.append(pltpu.make_async_copy(
                    arrays[n].at[pl.ds(at * 64, 64)],
                    wd.at[xs % 2, pl.ds(row, 64), pl.ds(which * 768, 768)], sems.at[len(copies)]))
    for cp in copies:
        cp.start()
    for cp in copies:
        cp.wait()

    def rows(m, _):
        r = pl.ds(pl.multiple_of(m * 256, 256), 256)
        swapped = jnp.concatenate(
            [other[pl.ds(pl.multiple_of(m * 256 + at, 64), 64), :] for at in (64, 0, 192, 128)], axis=0)
        h = [jnp.concatenate([own[r, pl.ds(p * 256, 256)], swapped[:, p * 256:p * 256 + 256]], axis=1) for p in range(2)]
        s = jnp.dot(h[0], wd[0], preferred_element_type=F32) + jnp.dot(h[1], wd[1], preferred_element_type=F32)
        out[r, :] = s.astype(BF)
        return _

    lax.fori_loop(0, 4, rows, 0)


def call(kernel, pos, vmem, hbm, out_shape, scratch, flops, name):
    return pl.pallas_call(
        kernel,
        out_shape=jax.ShapeDtypeStruct(out_shape, BF),
        in_specs=[pl.BlockSpec(memory_space=pltpu.SMEM)]
        + [pl.BlockSpec(memory_space=pltpu.VMEM)] * len(vmem)
        + [pl.BlockSpec(memory_space=pl.ANY)] * len(hbm),
        out_specs=pl.BlockSpec(memory_space=pltpu.VMEM),
        scratch_shapes=[pltpu.VMEM(s, BF) for s in scratch] + [pltpu.SemaphoreType.DMA((32,))],
        compiler_params=pltpu.CompilerParams(vmem_limit_bytes=48 * 1024 * 1024),
        cost_estimate=pl.CostEstimate(flops=flops, bytes_accessed=12 << 20, transcendentals=0),
        name=name,
    )(pos, *vmem, *hbm)


def on_device(tokens, expert_ids, gate_num, gate_weight, up_weight, down_weight):
    blk, dp = lax.axis_index("blk"), lax.axis_index("dp")
    core = dp % 2
    x = dp // 8 * 2 + blk // 8
    y = dp // 2 % 4
    pos = jnp.stack([x, y, core]).astype(jnp.int32)
    even = core == 0

    both = jnp.concatenate([gate_weight, up_weight], axis=1)
    weights_xy = lax.all_gather(both, AXES, axis_index_groups=PLANES, axis=0, tiled=True)

    keep = lax.dynamic_slice_in_dim(down_weight, core * 1536, 1536, 1)
    got = shift(lax.dynamic_slice_in_dim(down_weight, (1 - core) * 1536, 1536, 1), other_core=True)
    down = jnp.concatenate([jnp.where(even, keep, got), jnp.where(even, got, keep)], axis=0)

    def bundle(r):
        return jnp.concatenate(r, axis=0)

    down_a = ring4(bundle(ring4(down[:, :768], "dx", 32)), "dy", 128)
    down_b = ring4(bundle(ring4(down[:, 768:], "dy", 32)), "dx", 128)

    marks = route_table(expert_ids, 64)
    packed = lax.dot_general(
        marks, tokens, (((0,), (0,)), ((), ())), preferred_element_type=F32
    ).astype(BF)
    below, above = [packed], [packed]
    for s in range(3):
        below.append(shift(below[-1], dz=1))
        above.append(shift(above[-1], dz=-1))
    far_a = shift(below[3][:32], dz=1)
    far_b = shift(above[3][32:], dz=-1)
    chunks = [[far_a, far_b], [above[3]], [below[3]], [above[2]], [below[2]], [above[1]], [below[1]], [packed]]
    rows = []
    for chunk in chunks:
        rows += chunk + [shift(a, other_core=True) for a in chunk]
    together = jnp.concatenate(rows, axis=0)

    hidden = call(hidden_kernel, pos, [together], [weights_xy], (1024, 512), [(2, 3072, 512)],
                  2 * 1024 * 3072 * 1024, "hidden")
    other = shift(hidden, other_core=True)
    term = call(down_kernel, pos, [hidden, other], list(down_a + down_b), (1024, 1536), [(2, 512, 1536)],
                2 * 1024 * 1024 * 1536, "down")

    def part(i):
        return term[128 * i:128 * i + 128].astype(F32)

    up_sum = shift(term[:64], dz=1)
    down_sum = shift(term[64:128], dz=-1)
    pad = jnp.zeros((64, 1536), BF)
    up_sum = jnp.concatenate([up_sum, pad], axis=0)
    down_sum = jnp.concatenate([pad, down_sum], axis=0)
    for s in range(3):
        up_sum, down_sum = lax.optimization_barrier((
            (part(1 + 2 * s) + up_sum.astype(F32)).astype(BF), (part(2 + 2 * s) + down_sum.astype(F32)).astype(BF)))
        up_sum, down_sum = shift(up_sum, dz=1), shift(down_sum, dz=-1)
    total = (part(7) + up_sum.astype(F32) + down_sum.astype(F32)).astype(BF)
    mine = total[:64]
    theirs = shift(total[64:], other_core=True)
    own_rows = jnp.concatenate([jnp.where(even, mine, theirs), jnp.where(even, theirs, mine)], axis=1)
    expanded = jnp.dot(marks, own_rows, preferred_element_type=F32)
    weights = gate_values(expert_ids, gate_num)
    return (weights[:, None] * expanded).astype(BF)


def solution(mesh):
    return jax.shard_map(
        on_device,
        mesh=mesh,
        in_specs=(
            P(("blk", "dp"), None),
            P(("blk", "dp"), None),
            P(("blk", "dp")),
            P("dp", "blk"),
            P("dp", "blk"),
            P(("blk", "dp"), None),
        ),
        out_specs=P(("blk", "dp"), None),
        check_vma=False,
    )
```

```python
import jax
import jax.numpy as jnp
from jax import lax
from jax.experimental import pallas as pl
from jax.experimental.pallas import tpu as pltpu
from jax.sharding import PartitionSpec as P

GATE_SCALE = 256.0
AXES = ("blk", "dp")
BF = jnp.bfloat16
F32 = jnp.float32

NX, NY, NZ = 4, 4, 8


def shift(a, dx=0, dy=0, dz=0, other_core=False):
    pairs = []
    for i in range(256):
        xl, z, xh, y, c = i // 128, i // 16 % 8, i // 8 % 2, i // 2 % 4, i % 2
        x = (2 * xh + xl + dx) % NX
        y = (y + dy) % NY
        z = (z + dz) % NZ
        c = 1 - c if other_core else c
        pairs.append((i, (x % 2) * 128 + z * 16 + (x // 2) * 8 + y * 2 + c))
    return lax.ppermute(a, AXES, pairs)


def device(xl, z, xh, y, c):
    return xl * 128 + z * 16 + xh * 8 + y * 2 + c


PLANES = [
    [device(x % 2, z, x // 2, y, c) for x in range(4) for y in range(4) for c in range(2)] for z in range(8)
]


def route_table(expert_ids, slot_count):
    hits = jnp.sum((expert_ids == 0).astype(jnp.int32), axis=1)
    position = jnp.cumsum(hits) - 1
    marks = (hits[:, None] > 0) & (
        position[:, None] == jnp.arange(slot_count, dtype=jnp.int32)[None, :]
    )
    return marks.astype(BF)


def gate_values(expert_ids, gate_num):
    first = gate_num.astype(F32) / GATE_SCALE
    return jnp.where(expert_ids[:, 0] == 0, first, 0.0) + jnp.where(
        expert_ids[:, 1] == 0, 1.0 - first, 0.0
    )


def ring4(a, axis, cut):
    low = shift(a, **{axis: 1})
    high = shift(a, **{axis: -1})
    far_a = shift(low[:cut], **{axis: 1})
    far_b = shift(high[cut:], **{axis: -1})
    return a, low, far_a, far_b, high


RING_PARTS = ((0, 0, (0, 1, 2, 3)), (1, 1, (0, 1, 2, 3)), (2, 2, (0, 1)), (3, 2, (2, 3)), (4, 3, (0, 1, 2, 3)))
STEPS = (0, -1, 2, 1)


def hidden_kernel(pos, weights, *refs):
    pieces = refs[:18]
    out, tok, w, sems, wsems = refs[18:]
    c = pos[2]
    copies = []
    for xl in range(2):
        for which in range(2):
            col = pl.multiple_of(which * 512 + c * 256, 256)
            for xh in range(2):
                copies.append(pltpu.make_async_copy(
                    weights.at[pl.ds((xh * 2 + xl) * 1536, 1536), pl.ds(col, 256)],
                    w.at[xl, pl.ds(xh * 1536, 1536), pl.ds(which * 256, 256)], wsems.at[len(copies)]))
    loads, at = [], 0
    for piece in pieces:
        loads.append(pltpu.make_async_copy(
            piece, tok.at[pl.ds(at, piece.shape[0])], sems.at[len(loads)]))
        at += piece.shape[0]
    for cp in copies[:4] + loads + copies[4:]:
        cp.start()

    def rows(xl, m):
        r = pl.ds(m * 512, 512)
        s = jnp.dot(tok[r, :], w[xl], preferred_element_type=F32)
        g, u = s[:, :256], s[:, 256:]
        out[r, pl.ds(xl * 256, 256)] = (g / (1.0 + jnp.exp(-g)) * u).astype(BF)

    for cp in copies[:4] + loads[:10]:
        cp.wait()
    rows(0, 0)
    for cp in loads[10:]:
        cp.wait()
    rows(0, 1)
    for cp in copies[4:]:
        cp.wait()
    rows(1, 0)
    rows(1, 1)


def down_kernel(pos, own, other, *refs):
    arrays = refs[:5]
    out, wd, sems = refs[5:]
    x, y, c = pos[0], pos[1], pos[2]
    copies = []
    for n, j, inner in RING_PARTS:
        for at, i in enumerate(inner):
            xs, ys = (x + STEPS[i]) % NX, (y + STEPS[j]) % NY
            row = pl.multiple_of(jnp.where(xs // 2 == c, 0, 256) + ys * 64, 64)
            copies.append(pltpu.make_async_copy(
                arrays[n].at[pl.ds(at * 64, 64)], wd.at[xs % 2, pl.ds(row, 64)], sems.at[len(copies)]))
    for cp in copies:
        cp.start()
    for cp in copies:
        cp.wait()

    def rows(m, _):
        r = pl.ds(pl.multiple_of(m * 256, 256), 256)
        swapped = jnp.concatenate(
            [other[pl.ds(pl.multiple_of(m * 256 + at, 64), 64), :] for at in (64, 0, 192, 128)], axis=0)
        h = [jnp.concatenate([own[r, pl.ds(p * 256, 256)], swapped[:, p * 256:p * 256 + 256]], axis=1) for p in range(2)]
        s = jnp.dot(h[0], wd[0], preferred_element_type=F32) + jnp.dot(h[1], wd[1], preferred_element_type=F32)
        out[r, :] = s.astype(BF)
        return _

    lax.fori_loop(0, 4, rows, 0)


def call(kernel, pos, vmem, hbm, out_shape, scratch, flops, sems, name):
    return pl.pallas_call(
        kernel,
        out_shape=jax.ShapeDtypeStruct(out_shape, BF),
        in_specs=[pl.BlockSpec(memory_space=pltpu.SMEM)]
        + [pl.BlockSpec(memory_space=pltpu.VMEM)] * len(vmem)
        + [pl.BlockSpec(memory_space=pl.ANY)] * len(hbm),
        out_specs=pl.BlockSpec(memory_space=pltpu.VMEM),
        scratch_shapes=[pltpu.VMEM(s, BF) for s in scratch] + [pltpu.SemaphoreType.DMA((n,)) for n in sems],
        compiler_params=pltpu.CompilerParams(vmem_limit_bytes=48 * 1024 * 1024),
        cost_estimate=pl.CostEstimate(flops=flops, bytes_accessed=12 << 20, transcendentals=0),
        name=name,
    )(pos, *vmem, *hbm)


def on_device(tokens, expert_ids, gate_num, gate_weight, up_weight, down_weight):
    blk, dp = lax.axis_index("blk"), lax.axis_index("dp")
    core = dp % 2
    x = dp // 8 * 2 + blk // 8
    y = dp // 2 % 4
    pos = jnp.stack([x, y, core]).astype(jnp.int32)
    even = core == 0

    both = jnp.concatenate([gate_weight, up_weight], axis=1)
    weights_xy = lax.all_gather(both, AXES, axis_index_groups=PLANES, axis=0, tiled=True)

    keep = lax.dynamic_slice_in_dim(down_weight, core * 1536, 1536, 1)
    got = shift(lax.dynamic_slice_in_dim(down_weight, (1 - core) * 1536, 1536, 1), other_core=True)
    down = jnp.concatenate([jnp.where(even, keep, got), jnp.where(even, got, keep)], axis=0)

    downs = ring4(jnp.concatenate(ring4(down, "dx", 32), axis=0), "dy", 128)

    marks = route_table(expert_ids, 64)
    packed = lax.dot_general(
        marks, tokens, (((0,), (0,)), ((), ())), preferred_element_type=F32
    ).astype(BF)
    below, above = [packed], [packed]
    for s in range(3):
        below.append(shift(below[-1], dz=1))
        above.append(shift(above[-1], dz=-1))
    far_a = shift(below[3][:32], dz=1)
    far_b = shift(above[3][32:], dz=-1)
    chunks = [[far_a, far_b], [above[3]], [below[3]], [above[2]], [below[2]], [above[1]], [below[1]], [packed]]
    rows = []
    for chunk in chunks:
        rows += chunk + [shift(a, other_core=True) for a in chunk]
    weights_xy, downs = lax.optimization_barrier((weights_xy, downs))
    hidden = call(hidden_kernel, pos, [], [weights_xy] + rows, (1024, 512), [(1024, 3072), (2, 3072, 512)],
                  2 * 1024 * 3072 * 1024, (18, 8), "hidden")
    other = shift(hidden, other_core=True)
    term = call(down_kernel, pos, [hidden, other], list(downs), (1024, 1536), [(2, 512, 1536)],
                2 * 1024 * 1024 * 1536, (16,), "down")

    def part(i):
        return term[128 * i:128 * i + 128].astype(F32)

    up_sum = shift(term[:64], dz=1)
    down_sum = shift(term[64:128], dz=-1)
    pad = jnp.zeros((64, 1536), BF)
    up_sum = jnp.concatenate([up_sum, pad], axis=0)
    down_sum = jnp.concatenate([pad, down_sum], axis=0)
    for s in range(3):
        up_sum, down_sum = lax.optimization_barrier((
            (part(1 + 2 * s) + up_sum.astype(F32)).astype(BF), (part(2 + 2 * s) + down_sum.astype(F32)).astype(BF)))
        up_sum, down_sum = shift(up_sum, dz=1), shift(down_sum, dz=-1)
    total = (part(7) + up_sum.astype(F32) + down_sum.astype(F32)).astype(BF)
    mine = total[:64]
    theirs = shift(total[64:], other_core=True)
    own_rows = jnp.concatenate([jnp.where(even, mine, theirs), jnp.where(even, theirs, mine)], axis=1)
    expanded = jnp.dot(marks, own_rows, preferred_element_type=F32)
    weights = gate_values(expert_ids, gate_num)
    return (weights[:, None] * expanded).astype(BF)


def solution(mesh):
    return jax.shard_map(
        on_device,
        mesh=mesh,
        in_specs=(
            P(("blk", "dp"), None),
            P(("blk", "dp"), None),
            P(("blk", "dp")),
            P("dp", "blk"),
            P("dp", "blk"),
            P(("blk", "dp"), None),
        ),
        out_specs=P(("blk", "dp"), None),
        check_vma=False,
    )
```
